32 devices in a mesh: groups: 2 (over x), wide: 16 (over z, y, core).
Axes of the slice: x: 2, y: 2, z: 4, core: 2. Of those that a mesh axis runs over, the one named last changes fastest.
Arguments:
- queries: bfloat16 [256, 3072], P(('groups', 'wide')), parts along dimension 0, may hold values from -15 to 15
- hidden_in: bfloat16 [256, 3072], P(('groups', 'wide')), parts along dimension 0, may hold values from -170 to 170
- prefix_keys: bfloat16 [16384, 512], P(('groups', 'wide')), parts along dimension 0, may hold values from -12 to 12
- prefix_values: bfloat16 [16384, 512], P(('groups', 'wide')), parts along dimension 0, may hold values from -24 to 24
- suffix_keys: bfloat16 [256, 64, 512], P(('groups', 'wide')), parts along dimension 0, may hold values from -21 to 21
- suffix_values: bfloat16 [256, 64, 512], P(('groups', 'wide')), parts along dimension 0, may hold values from -24 to 24
- suffix_length: int32 [256], P(('groups', 'wide')), parts along dimension 0, may hold values from 2 to 64, as said below
- prefix_of: int32 [256, 1], P('groups'), parts along dimension 0, may hold values from 0 to 7; in each aligned block of 8 rows (0 to 7, 8 to 15, ...) at most 2 rows name the same one
- expert_index: int32 [256, 2], P('groups'), parts along dimension 0, may hold values from 0 to 3, all different within a row; in each aligned block of 8 rows (0 to 7, 8 to 15, ...) at most 6 rows name the same one
- gate_logits: float32 [256, 2], P('groups'), parts along dimension 0, may hold values from -6 to 6
- norm_gain: float32 [3072], replicated, may hold values from 0.1 to 1.9
- gate_weight: bfloat16 [3072, 32768], P(None, 'wide'), may hold values from -0.109375 to 0.109375
- up_weight: bfloat16 [3072, 32768], P(None, 'wide'), may hold values from -0.109375 to 0.109375
- down_weight: bfloat16 [32768, 3072], P('wide'), may hold values from -0.125 to 0.125
Outputs:
- attended: bfloat16 [256, 3072], P(('groups', 'wide')), parts along dimension 0
- expert_mix: bfloat16 [256, 3072], P(('groups', 'wide')), parts along dimension 0
The draws below stay inside these ranges and needn't reach their ends.
There are 2 independent parts, one for each index of `groups`. The reference program is written for one: setup_inputs(seed, part) draws one part's arguments, and reference() takes and returns one part's arrays. A program takes and returns all parts, laid end to end along the dimension named above; an argument that names none is the same for every part. Nothing has to cross between parts.
Inputs may be any that keep to these rules, and one draw needn't show every extreme that they name: `prefix_of`: among the requests of one device at most 2 share a prefix; in some of the aligned blocks exactly 2 do. `expert_index`: each request names 2 different experts; among the requests of one device at most 6 name the same expert, and in some aligned blocks exactly 6 do. `suffix_length`: every device holds a request with 64 live suffix tokens.
All inputs are finite; a program needn't handle non-finite values.
Results may differ from the reference program's by a relative error of at most 0.0095.
Values may be sent and summed in bfloat16 or wider, within the bound.
A program may use at most 128 MiB of HBM per device.

```python
import math
import jax
import jax.numpy as jnp
import numpy as np
from jax import lax

D = 3072
HQ = 24
HK = 4
DH = 128
FF = 8192
EXPERTS = 4
TOP = 2
PREFIXES = 8
PTOK_DEV = 512
REQ_DEV = 8
SMAX = 64
CAPP = 2
CAPE = 6
R = 128
PLEN = 1024


def draw_queries(key, part):
    values_out = jnp.clip(jax.random.normal(jax.random.fold_in(key, 11), (R, D), jnp.float32), -4.0, 4.0)
    return values_out.astype(jnp.bfloat16)


def draw_suffix_keys(key, part):
    values_out = jnp.clip(2.0 * jax.random.normal(jax.random.fold_in(key, 21), (R, SMAX, HK * DH), jnp.float32), -12.0, 12.0)
    return values_out.astype(jnp.bfloat16)


def draw_suffix_length(key, part):
    lengths = jax.random.randint(jax.random.fold_in(key, 31), (R,), 2, SMAX + 1)
    picked = jax.random.randint(jax.random.fold_in(key, 32), (R // REQ_DEV,), 0, REQ_DEV)
    position = jnp.arange(R)
    longest = position % REQ_DEV == picked[position // REQ_DEV]
    return jnp.where(longest, SMAX, lengths).astype(jnp.int32)


def draw_hidden_in(key, part):
    values_out = jnp.clip(jax.random.normal(jax.random.fold_in(key, 41), (R, D), jnp.float32), -5.0, 5.0)
    return values_out.astype(jnp.bfloat16)


def levels(own_key, shape, pieces, least, top_value):
    level = 1.0
    for dim, shards_of in pieces:
        draws = jax.random.uniform(jax.random.fold_in(jax.random.fold_in(own_key, 6), dim), (shards_of,), jnp.float32, least / len(pieces), top_value / len(pieces))
        level = level * jnp.repeat(jnp.exp(draws), shape[dim] // shards_of).reshape((-1,) + (1,) * (len(shape) - 1 - dim))
    return level


def deal_out(rng, own, number, rows, number_of, top, bound, skew):
    order = jax.random.permutation(rng, number_of)
    crowded, common = load_shares(number_of, rows * top, bound, skew, True), load_shares(number_of, rows * top, bound, skew, False)
    places = jnp.arange(number_of)

    def named(sizes, rotation):
        used = int((sizes > 0).sum())
        fixed = max(1, used // 4)
        shifted = fixed + (places - fixed + rotation * (used - fixed)) % max(1, number_of - fixed)
        return jnp.zeros((number_of,), jnp.int32).at[order[jnp.where(places < fixed, places, shifted)]].set(jnp.asarray(sizes, jnp.int32))

    sizes = jnp.where(number % 4 == 0, named(crowded, number // 4), named(common, number - number // 4 - 1))
    mixed = jax.random.permutation(jax.random.fold_in(own, 3), number_of)
    source_of, sink = mixed[0:number_of // 2 * 2:2], mixed[1:number_of // 2 * 2:2]
    slack = jnp.minimum(sizes[source_of] - 1, bound - sizes[sink]) // 2
    slack = jnp.where((source_of == order[0]) | (sink == order[0]) | (sizes[sink] == 0), 0, jnp.maximum(slack, 0))
    shifted = jax.random.randint(jax.random.fold_in(own, 4), (number_of // 2,), 0, 1 << 20) % (slack + 1)
    sizes = sizes.at[source_of].add(-shifted).at[sink].add(shifted)
    labels = jnp.searchsorted(jnp.cumsum(sizes), jnp.arange(rows * top), side="right").astype(jnp.int32)
    grid = labels.reshape(top, rows).T
    grid = grid[jax.random.permutation(jax.random.fold_in(own, 1), rows)]
    rotation = jax.random.randint(jax.random.fold_in(own, 2), (rows, 1), 0, top)
    return jnp.take_along_axis(grid, (jnp.arange(top)[None, :] + rotation) % top, axis=1)


def load_shares(count, total, most, slope, full):
    loads = [(1 << 20) // math.isqrt(grade ** slope) + 1 for grade in range(1, count + 1)]
    largest = most if full else min(most, max(-(-total // count), total * loads[0] // sum(loads)))
    least = 1 if total - largest >= count - 1 else 0
    counts, spare = [largest] + [least] * (count - 1), total - largest - least * (count - 1)
    while spare > 0:
        movable = [i for i in range(1, count) if counts[i] < largest] or [i for i in range(1, count) if counts[i] < most]
        pool, left = sum([loads[i] for i in movable]), spare
        for i in movable:
            more = min(most - counts[i], max(1, left * loads[i] // pool), spare)
            counts[i] = counts[i] + more
            spare = spare - more
    return np.array(counts)


def bell_draw(rng, shape, deviation, most, pieces=(), held_as=jnp.bfloat16):
    result = deviation * jax.random.normal(rng, shape, jnp.float32)
    if pieces:
        result = result * levels(rng, shape, pieces, -0.22, 0.18)
    return jnp.clip(result, -most, most).astype(held_as)


def setup_inputs(seed: int = 0, part: int = 0) -> dict:
    key_list = jax.random.split(jax.random.key(seed), 15)
    part_splits = jax.random.split(jax.random.fold_in(key_list[14], part), 15)
    queries = draw_queries(jax.random.fold_in(jax.random.fold_in(key_list[14], part), 71), part)
    hidden_in = draw_hidden_in(jax.random.fold_in(jax.random.fold_in(key_list[14], part), 71), part)
    prefix_keys = bell_draw(part_splits[2], (PREFIXES * PLEN, HK * DH), 2.0, 12.0, ((0, 16),))
    prefix_values = bell_draw(part_splits[3], (PREFIXES * PLEN, HK * DH), 4.0, 24.0, ((0, 16),))
    suffix_keys = draw_suffix_keys(jax.random.fold_in(jax.random.fold_in(key_list[14], part), 71), part)
    suffix_values = bell_draw(part_splits[5], (R, SMAX, HK * DH), 4.0, 24.0, ((0, 16),))
    suffix_length = draw_suffix_length(jax.random.fold_in(jax.random.fold_in(key_list[14], part), 71), part)
    prefix_of_keys = jax.random.split(jax.random.fold_in(part_splits[7], 1), R // REQ_DEV)
    prefix_of_turns = jax.random.permutation(jax.random.fold_in(part_splits[7], 3), R // REQ_DEV)
    prefix_of = jax.vmap(lambda own, number: deal_out(jax.random.fold_in(part_splits[7], 2), own, number, REQ_DEV, PREFIXES, 1, CAPP, 2))(prefix_of_keys, prefix_of_turns).reshape((R, 1))
    expert_index_keys = jax.random.split(jax.random.fold_in(part_splits[8], 1), R // REQ_DEV)
    expert_index_turns = jax.random.permutation(jax.random.fold_in(part_splits[8], 3), R // REQ_DEV)
    expert_index = jax.vmap(lambda own, number: deal_out(jax.random.fold_in(part_splits[8], 2), own, number, REQ_DEV, EXPERTS, TOP, CAPE, 2))(expert_index_keys, expert_index_turns).reshape((R, TOP))
    gate_logits = bell_draw(part_splits[9], (R, TOP), 1.0, 6.0, (), jnp.float32)
    norm_gain = jnp.clip(1.0 + 0.18 * jax.random.normal(key_list[10], (D,), jnp.float32), 0.1, 1.9)
    gate_weight = bell_draw(key_list[11], (D, EXPERTS * FF), D ** -0.5, 0.109375, ((1, 16),))
    up_weight = bell_draw(key_list[12], (D, EXPERTS * FF), D ** -0.5, 0.109375, ((1, 16),))
    down_weight = bell_draw(key_list[13], (EXPERTS * FF, D), (FF // 4) ** -0.5, 0.125, ((0, 16),))
    return dict(queries=queries, hidden_in=hidden_in, prefix_keys=prefix_keys, prefix_values=prefix_values, suffix_keys=suffix_keys, suffix_values=suffix_values, suffix_length=suffix_length, prefix_of=prefix_of, expert_index=expert_index, gate_logits=gate_logits, norm_gain=norm_gain, gate_weight=gate_weight, up_weight=up_weight, down_weight=down_weight)


masked_score = -1e+30

def reference(queries, hidden_in, prefix_keys, prefix_values, suffix_keys, suffix_values, suffix_length, prefix_of, expert_index, gate_logits, norm_gain, gate_weight, up_weight, down_weight):
    group_size = HQ // HK
    blocks = PLEN // PTOK_DEV
    score_scale = 1.0 / math.sqrt(DH)

    def one_request(packed):
        query_row, prefix_row, own_keys, own_values, length = packed
        query_heads = query_row.astype(jnp.float32).reshape(HK, group_size, DH)
        first_row = (prefix_row * PLEN).astype(jnp.int32)
        prefix_k = lax.dynamic_slice_in_dim(prefix_keys, first_row, PLEN, 0).astype(jnp.float32).reshape(blocks, PTOK_DEV, HK, DH)
        prefix_v = lax.dynamic_slice_in_dim(prefix_values, first_row, PLEN, 0).astype(jnp.float32).reshape(blocks, PTOK_DEV, HK, DH)
        scores = jnp.einsum('kgd,btkd->kgbt', query_heads, prefix_k) * score_scale
        block_max = lax.optimization_barrier(jnp.max(scores, axis=-1))
        weights = lax.optimization_barrier(jnp.exp(scores - block_max[..., None]).astype(jnp.bfloat16)).astype(jnp.float32)
        block_sum = lax.optimization_barrier(jnp.sum(weights, axis=-1))
        block_out = jnp.einsum('kgbt,btkd->kgbd', weights, prefix_v)
        suffix_k = own_keys.astype(jnp.float32).reshape(SMAX, HK, DH)
        suffix_v = own_values.astype(jnp.float32).reshape(SMAX, HK, DH)
        suffix_scores = jnp.einsum('kgd,skd->kgs', query_heads, suffix_k) * score_scale
        usable = jnp.arange(SMAX, dtype=jnp.int32) < length
        suffix_scores = jnp.where(usable, suffix_scores, masked_score)
        suffix_max = lax.optimization_barrier(jnp.max(suffix_scores, axis=-1))
        suffix_weights = lax.optimization_barrier(jnp.exp(suffix_scores - suffix_max[..., None]).astype(jnp.bfloat16)).astype(jnp.float32)
        suffix_sum = lax.optimization_barrier(jnp.sum(suffix_weights, axis=-1))
        suffix_out = jnp.einsum('kgs,skd->kgd', suffix_weights, suffix_v)
        overall = jnp.maximum(lax.optimization_barrier(jnp.max(block_max, axis=-1)), suffix_max)
        factors = jnp.exp(block_max - overall[..., None])
        suffix_factor = jnp.exp(suffix_max - overall)
        numerator = lax.optimization_barrier(jnp.sum(factors[..., None] * block_out, axis=2)) + suffix_factor[..., None] * suffix_out
        denominator = lax.optimization_barrier(jnp.sum(factors * block_sum, axis=-1)) + suffix_factor * suffix_sum
        return (numerator / denominator[..., None]).reshape(D).astype(jnp.bfloat16)
    attended = lax.map(one_request, (queries, prefix_of[:, 0], suffix_keys, suffix_values, suffix_length))
    stream = hidden_in.astype(jnp.float32) + attended.astype(jnp.float32)
    normed = (stream * lax.rsqrt(lax.optimization_barrier(jnp.mean(stream * stream, axis=-1, keepdims=True)) + 1e-05) * norm_gain).astype(jnp.bfloat16)
    gates = jax.nn.softmax(gate_logits, axis=-1)
    mixture = jnp.zeros((R, D), jnp.float32)
    for expert in range(EXPERTS):
        gate_part = jnp.dot(normed, gate_weight[:, expert * FF:(expert + 1) * FF], preferred_element_type=jnp.float32)
        up_part = jnp.dot(normed, up_weight[:, expert * FF:(expert + 1) * FF], preferred_element_type=jnp.float32)
        hidden = (jax.nn.silu(gate_part) * up_part).astype(jnp.bfloat16)
        expert_out = jnp.dot(hidden, down_weight[expert * FF:(expert + 1) * FF, :], preferred_element_type=jnp.float32)
        share = lax.optimization_barrier(jnp.sum(gates * (expert_index == expert).astype(jnp.float32), axis=1))
        mixture = mixture + share[:, None] * expert_out
    return (attended, mixture.astype(jnp.bfloat16))
```

```python
import functools
import math

import jax
import jax.numpy as jnp
from jax import lax
from jax.experimental import pallas as pl
from jax.experimental.pallas import tpu as pltpu
from jax.sharding import PartitionSpec as P

HQ = 24
HK = 4
DH = 128
EXPERTS = 4
PREFIXES = 8
CAPP = 2
GROUP = HQ // HK
GPAD = 8

masked_score = -1e30
F32 = jnp.float32
BF16 = jnp.bfloat16


def nt(a, b):
    return lax.dot_general(a, b, (((1,), (1,)), ((), ())), preferred_element_type=F32)


def softmax_block(scores, values):
    top = jnp.max(scores, axis=1, keepdims=True)
    weights = jnp.exp(scores - top).astype(BF16)
    total = jnp.sum(weights.astype(F32), axis=1, keepdims=True)
    out = jnp.dot(weights, values, preferred_element_type=F32)
    return out, top, total


def kernel(
    n,
    len_hbm,
    pref_hbm,
    q_hbm,
    hid_hbm,
    pk_hbm,
    pv_hbm,
    sk_hbm,
    sv_hbm,
    ei_hbm,
    gl_hbm,
    gain_hbm,
    wg_hbm,
    wu_hbm,
    wd_hbm,
    att_ref,
    mix_ref,
    q_ref,
    hid_ref,
    sk_ref,
    sv_ref,
    ei_ref,
    gl_ref,
    gain_ref,
    kx,
    vx,
    wg_v,
    wu_v,
    wd_v,
    qsend,
    qrecv,
    pout,
    bout,
    stream,
    x_v,
    h_v,
    dsend,
    drecv,
    keep,
    esend,
    erecv,
    keep2,
    zsend,
    zrecv,
    len_s,
    pref_s,
    in_sem,
    w_sem,
    kv_in,
    kv_ss,
    kv_rs,
    q_ss,
    q_rs,
    o_ss,
    o_rs,
    x_ss,
    x_rs,
    g_rs,
    d_ss,
    d_rs,
    e_ss,
    e_rs,
    z_ss,
    z_rs,
):
    me = lax.axis_index("wide")
    rows, width = q_ref.shape
    quads = n // 4
    parity = lax.rem(me, 2)
    half = lax.rem(me // 2, 2)
    quad = me // 4
    sib = me + 1 - 2 * parity
    pair = me + 2 - 4 * half
    heads = HK // 2
    chips_p = n // PREFIXES // 2
    hold_p = n // PREFIXES
    hold_e = n // EXPERTS
    slots = CAPP * GPAD
    up_chunks, _, up_cols = wg_v.shape
    down_chunks, _, down_cols = wd_v.shape
    scale = 1.0 / math.sqrt(DH)

    others, other_quads = pl.ds(0, n - 1), pl.ds(0, quads - 1)

    def send(src, dst, ss, rs, to):
        return pltpu.make_async_remote_copy(
            src_ref=src,
            dst_ref=dst,
            send_sem=ss,
            recv_sem=rs,
            device_id={"wide": to},
            device_id_type=pl.DeviceIdType.MESH,
        )

    barrier = pltpu.get_barrier_semaphore()

    upper = quad // (quads // 2)

    def far_quad(i):
        down = quads - 1 - i
        down = down - (quad - down + quads) // quads
        rise = i + (i - quad + quads) // quads
        return (1 - upper) * down + upper * rise

    def near_quad(i):
        return far_quad(quads - 2 - i)

    def for_others(act):
        @pl.loop(0, quads - 1)
        def _(i):
            first = 4 * far_quad(i)
            for k in range(4):
                act(first + lax.rem(2 * (1 - half) + k, 4))

        act(pair + 1 - 2 * parity)
        act(pair)
        act(sib)

    def greet(to):
        pl.semaphore_signal(
            barrier,
            inc=1,
            device_id={"wide": to},
            device_id_type=pl.DeviceIdType.MESH,
        )

    for_others(greet)
    scalars = [
        pltpu.make_async_copy(pref_hbm, pref_s, in_sem.at[7]),
        pltpu.make_async_copy(len_hbm, len_s, in_sem.at[8]),
    ]
    for copy in scalars:
        copy.start()

    ins = [
        pltpu.make_async_copy(src, dst, in_sem.at[i])
        for i, (src, dst) in enumerate(
            (
                (q_hbm, q_ref),
                (sk_hbm, sk_ref),
                (sv_hbm, sv_ref),
                (hid_hbm, hid_ref),
                (ei_hbm, ei_ref),
                (gl_hbm, gl_ref),
                (gain_hbm, gain_ref),
            )
        )
    ]
    for copy in ins:
        copy.start()

    tokens, span = pk_hbm.shape[0], heads * DH
    here = pl.ds(pl.multiple_of(parity * span, span), span)
    there = pl.ds(pl.multiple_of((1 - parity) * span, span), span)
    kv_own = [
        pltpu.make_async_copy(pk_hbm.at[:, here], kx.at[parity], kv_in),
        pltpu.make_async_copy(pv_hbm.at[:, here], vx.at[parity], kv_in),
    ]
    kv_sib = [
        send(pk_hbm.at[:, there], kx.at[parity], kv_ss, kv_rs, sib),
        send(pv_hbm.at[:, there], vx.at[parity], kv_ss, kv_rs, sib),
    ]
    for copy in kv_own:
        copy.start()

    def up_copy(j):
        cols = pl.ds(pl.multiple_of(j * up_cols, up_cols), up_cols)
        return (
            pltpu.make_async_copy(wg_hbm.at[:, cols], wg_v.at[j], w_sem.at[0]),
            pltpu.make_async_copy(wu_hbm.at[:, cols], wu_v.at[j], w_sem.at[1]),
        )

    def down_copy(j):
        cols = pl.ds(pl.multiple_of(j * down_cols, down_cols), down_cols)
        return pltpu.make_async_copy(wd_hbm.at[:, cols], wd_v.at[j], w_sem.at[2])

    @pl.loop(0, up_chunks)
    def _(j):
        a, b = up_copy(j)
        a.start()
        b.start()

    @pl.loop(0, down_chunks)
    def _(j):
        down_copy(j).start()

    for copy in scalars:
        copy.wait()
    m = GROUP * rows
    shape = (m, PREFIXES * slots)
    sub = lax.broadcasted_iota(jnp.int32, shape, 0)
    lane = lax.broadcasted_iota(jnp.int32, shape, 1)
    req = lax.rem(sub, rows)
    own = [pref_s[me * rows + j] for j in range(rows)]
    pcol = jnp.zeros(shape, jnp.int32)
    for j in range(rows):
        pcol = jnp.where(req == j, own[j], pcol)
    rank = jnp.zeros(shape, jnp.int32)
    for j in range(rows):
        rank = rank + jnp.where((pcol == own[j]) & (req > j), 1, 0)
    place = pcol * slots + rank * GPAD + lax.div(sub, rows)
    pick_f = jnp.where((lane == place) & (rank < CAPP), 1.0, 0.0)
    pick = pick_f.astype(BF16)

    ins[0].wait()
    q_heads = []
    for k in range(HK):
        parts = [
            q_ref[:, (k * GROUP + g) * DH : (k * GROUP + g + 1) * DH].astype(F32)
            for g in range(GROUP)
        ]
        qk = jnp.concatenate(parts, axis=0).astype(BF16)
        q_heads.append(qk)
        moved = lax.dot_general(
            pick, qk, (((0,), (0,)), ((), ())), preferred_element_type=F32
        )
        qsend[:, k // heads, k % heads] = moved.astype(BF16).reshape(
            PREFIXES, slots, DH
        )

    qrecv[me] = qsend[me // hold_p, parity]
    pl.semaphore_wait(barrier, n - 1)

    def q_copy(to):
        return send(
            qsend.at[to // hold_p, lax.rem(to, 2)],
            qrecv.at[me],
            q_ss,
            q_rs,
            to,
        )

    for_others(lambda to: q_copy(to).start())

    for copy in kv_sib:
        copy.start()

    keys = sk_ref.shape[0]
    smax = keys // rows
    s_sub = lax.broadcasted_iota(jnp.int32, (m, keys), 0)
    s_lane = lax.broadcasted_iota(jnp.int32, (m, keys), 1)
    s_req = lax.rem(s_sub, rows)
    limit = jnp.zeros((m, keys), jnp.int32)
    for j in range(rows):
        limit = jnp.where(s_req == j, j * smax + len_s[j], limit)
    usable = (s_lane >= s_req * smax) & (s_lane < limit)
    ins[1].wait()
    ins[2].wait()
    suffix = []
    for k in range(HK):
        head = slice(k * DH, (k + 1) * DH)
        scores = nt(q_heads[k], sk_ref[:, head]) * scale
        scores = jnp.where(usable, scores, masked_score)
        suffix.append(softmax_block(scores, sv_ref[:, head]))

    for copy in ins[3:]:
        copy.wait()
    logits = gl_ref[...]
    e = jnp.exp(logits - jnp.max(logits, axis=0, keepdims=True))
    gates = e / jnp.sum(e, axis=0, keepdims=True)
    mine = ei_ref[...] == me // hold_e
    share = jnp.sum(jnp.where(mine, gates, 0.0), axis=0, keepdims=True)
    share = jnp.broadcast_to(share, (DH, n * rows)).T[:, :1]

    send(qrecv.at[others], qrecv.at[others], q_ss, q_rs, sib).wait_recv()

    pltpu.make_async_copy(kx, kx, kv_in).wait()
    send(kx, kx, kv_ss, kv_rs, sib).wait_recv()

    total_rows = n * slots
    p_sub = lax.rem(lax.broadcasted_iota(jnp.int32, (total_rows, DH), 0), GPAD)
    p_lane = lax.broadcasted_iota(jnp.int32, (total_rows, DH), 1)
    groups = total_rows // GPAD
    for k in range(heads):
        head = slice(k * DH, (k + 1) * DH)
        queries = qrecv[:, k].reshape(total_rows, DH)
        out, top, total = softmax_block(
            nt(queries, kx[:, :, head].reshape(2 * tokens, DH)) * scale,
            vx[:, :, head].reshape(2 * tokens, DH),
        )
        out = out / total
        log_sum = top + jnp.log(total)
        high = log_sum.astype(BF16).astype(F32)
        rest = log_sum - high
        mid = rest.astype(BF16).astype(F32)
        low = rest - mid

        def row_of(first, second):
            spread = jnp.where(p_lane == p_sub, first, 0.0)
            spread = jnp.where(p_lane == p_sub + GPAD, second, spread)
            summed = jnp.sum(
                spread.reshape(groups, GPAD, DH), axis=1, keepdims=True
            )
            return jnp.broadcast_to(summed, (groups, GPAD, DH)).reshape(
                total_rows, DH
            )

        out = jnp.where(p_sub == GROUP, row_of(high, mid), out)
        out = jnp.where(p_sub == GROUP + 1, row_of(low, jnp.zeros_like(low)), out)
        pout[:, k] = out.astype(BF16).reshape(n, slots, DH)

    def o_copy(to):
        return send(pout.at[to], bout.at[me], o_ss, o_rs, to)

    for_others(lambda to: o_copy(to).start())

    bout[me] = pout[me]

    m_sub = lax.div(lax.broadcasted_iota(jnp.int32, (m, DH), 0), rows)
    m_lane = lax.broadcasted_iota(jnp.int32, (m, DH), 1)
    base = pcol * slots + rank * GPAD

    def pick_row(g):
        return jnp.where((lane == base + g) & (rank < CAPP), 1.0, 0.0).astype(BF16)

    pick_a, pick_b = pick_row(GROUP), pick_row(GROUP + 1)
    lanes_a = (m_lane == m_sub) | (m_lane == m_sub + GPAD)
    lanes_b = m_lane == m_sub

    send(bout.at[others], bout.at[others], o_ss, o_rs, sib).wait_recv()

    for k in range(HK):
        blocks = bout[:, k % heads].reshape(PREFIXES, chips_p, 2, slots, DH)
        out_s, top_s, sum_s = suffix[k]
        outs, logs = [], []
        overall = top_s
        for h in range(chips_p):
            block = blocks[:, h, k // heads].reshape(PREFIXES * slots, DH)
            outs.append(jnp.dot(pick, block, preferred_element_type=F32))
            row_a = jnp.dot(pick_a, block, preferred_element_type=F32)
            row_b = jnp.dot(pick_b, block, preferred_element_type=F32)
            logs.append(
                jnp.sum(
                    jnp.where(lanes_a, row_a, 0.0) + jnp.where(lanes_b, row_b, 0.0),
                    axis=1,
                    keepdims=True,
                )
            )
            overall = jnp.maximum(overall, logs[-1])
        f = jnp.exp(top_s - overall)
        num, den = f * out_s, f * sum_s
        for h in range(chips_p):
            f = jnp.exp(logs[h] - overall)
            num = num + f * outs[h]
            den = den + f
        result = num / den
        for g in range(GROUP):
            cols = slice((k * GROUP + g) * DH, (k * GROUP + g + 1) * DH)
            att = result[g * rows : (g + 1) * rows].astype(BF16)
            att_ref[:, cols] = att
            stream[:, cols] = hid_ref[:, cols].astype(F32) + att.astype(F32)

    s = stream[...]
    mean = jnp.mean(s * s, axis=1, keepdims=True)
    x_v[me] = (s * lax.rsqrt(mean + 1e-05) * gain_ref[...]).astype(BF16)

    def x_copy(i):
        to = 4 * far_quad(i) + 2 * half + parity
        return send(x_v.at[me], x_v.at[me], x_ss, x_rs.at[me // 2], to)

    def x_pair(src):
        return send(x_v.at[src], x_v.at[src], x_ss, x_rs.at[src // 2], pair)

    def x_sib(src):
        return send(x_v.at[src], x_v.at[src], x_ss, g_rs, sib)

    for i in range(quads - 1):
        x_copy(i).start()
    x_pair(me).start()
    x_sib(me).start()

    def from_pair(src):
        x_pair(src).wait_recv()
        x_sib(src).start()

    for i in range(quads - 1):
        src = 4 * near_quad(i) + 2 * half + parity
        x_pair(src).wait_recv()
        x_pair(src).start()
        x_sib(src).start()
        before = pair if i == 0 else 4 * near_quad(i - 1) + 2 * (1 - half) + parity
        from_pair(before)
    from_pair(4 * near_quad(quads - 2) + 2 * (1 - half) + parity)

    landed = x_v.at[pl.ds(0, 2 * quads)]
    send(landed, landed, x_ss, g_rs, sib).wait_recv()

    x = x_v[...].reshape(n * rows, width)
    pltpu.make_async_copy(wg_v, wg_v, w_sem.at[0]).wait()
    pltpu.make_async_copy(wu_v, wu_v, w_sem.at[1]).wait()

    @pl.loop(0, up_chunks)
    def _(j):
        gate = jnp.dot(x, wg_v[j], preferred_element_type=F32)
        up = jnp.dot(x, wu_v[j], preferred_element_type=F32)
        h_v[j] = (gate / (1.0 + jnp.exp(-gate)) * up).astype(BF16)

    pltpu.make_async_copy(wd_v, wd_v, w_sem.at[2]).wait()
    hidden = jnp.concatenate([h_v[j] for j in range(up_chunks)], axis=1)

    def d_copy(j):
        return send(dsend.at[j], drecv.at[j], d_ss, d_rs.at[j], sib)

    def e_copy(j):
        return send(esend.at[j], erecv.at[j], e_ss, e_rs.at[j], pair)

    def z_copy(j, d):
        other = lax.rem(quad + d, quads)
        return send(
            zsend.at[j, other],
            zrecv.at[j, quad],
            z_ss,
            z_rs.at[j],
            4 * other + 2 * half + parity,
        )

    def second(j):
        d_copy(j).wait_recv()
        both = keep[j] + drecv[j].astype(F32)
        low = half == 0
        keep2[j] = jnp.where(low, both[:, 0], both[:, 1])
        esend[j] = jnp.where(low, both[:, 1], both[:, 0]).astype(BF16)
        e_copy(j).start()

    def third(j):
        e_copy(j).wait_recv()
        zsend[j] = (keep2[j] + erecv[j].astype(F32)).astype(BF16)

        @pl.loop(1, quads)
        def _(d):
            z_copy(j, d).start()

        zrecv[j, quad] = zsend[j, quad]

    @pl.loop(0, down_chunks)
    def _(j):
        y = jnp.dot(hidden, wd_v[j], preferred_element_type=F32) * share
        y = y.reshape(quads, 2, 2, rows, down_cols)
        even = parity == 0
        keep[j] = jnp.where(even, y[:, :, 0], y[:, :, 1])
        dsend[j] = jnp.where(even, y[:, :, 1], y[:, :, 0]).astype(BF16)
        d_copy(j).start()

        @pl.when(j > 1)
        def _():
            second(j - 2)

    second(down_chunks - 2)
    third(0)
    second(down_chunks - 1)

    @pl.loop(1, down_chunks)
    def _(j):
        third(j)

    for j in range(down_chunks):
        arrived = zrecv.at[j, other_quads]
        send(arrived, arrived, z_ss, z_rs.at[j], sib).wait_recv()
        total = jnp.sum(zrecv[j].astype(F32), axis=0)
        mix_ref[:, j * down_cols : (j + 1) * down_cols] = total.astype(BF16)

    send(kx, kx, kv_ss, kv_rs, sib).wait_send()
    send(qrecv.at[others], qrecv.at[others], q_ss, q_rs, sib).wait_send()
    send(bout.at[others], bout.at[others], o_ss, o_rs, sib).wait_send()
    send(x_v.at[others], x_v.at[others], x_ss, g_rs, sib).wait_send()
    send(dsend, drecv, d_ss, d_rs.at[0], sib).wait_send()
    send(esend, erecv, e_ss, e_rs.at[0], sib).wait_send()
    z_all = zsend.at[:, other_quads]
    send(z_all, z_all, z_ss, z_rs.at[0], sib).wait_send()


def hand_over(a_ref, b_ref, c_ref, d_ref):
    c_ref[...] = a_ref[...]
    d_ref[...] = b_ref[...]


def divisor(size, most):
    while size % most:
        most //= 2
    return most


def local(
    queries,
    hidden_in,
    prefix_keys,
    prefix_values,
    suffix_keys,
    suffix_values,
    suffix_length,
    prefix_of,
    expert_index,
    gate_logits,
    norm_gain,
    gate_weight,
    up_weight,
    down_weight,
):
    n = lax.axis_size("wide")
    rows, width = queries.shape
    hidden = gate_weight.shape[1]
    quads, heads = n // 4, HK // 2
    slots = CAPP * GPAD
    up_cols, down_cols = divisor(hidden, 256), divisor(width, 512)
    ups, downs = hidden // up_cols, width // down_cols
    vmem = pl.BlockSpec(memory_space=pltpu.VMEM)
    hbm = pl.BlockSpec(memory_space=pltpu.HBM)
    dma = pltpu.SemaphoreType.DMA
    kv = suffix_keys.shape[2]
    shapes = (
        jax.ShapeDtypeStruct((rows, width), BF16),
        jax.ShapeDtypeStruct((rows, width), BF16),
    )
    landing = tuple(pltpu.VMEM(a.shape, a.dtype) for a in shapes)
    operands = (
        queries,
        hidden_in,
        prefix_keys,
        prefix_values,
        suffix_keys.reshape(-1, kv),
        suffix_values.reshape(-1, kv),
        expert_index.T,
        gate_logits.T,
        norm_gain.reshape(1, -1),
        gate_weight,
        up_weight,
        down_weight,
    )
    landed = [operands[i] for i in (0, 1, 4, 5, 6, 7, 8)]
    placed = [
        pltpu.with_memory_space_constraint(a, pltpu.HBM)
        for a in (suffix_length, prefix_of.reshape(-1), *operands)
    ]
    pieces = (downs, quads, rows, down_cols)
    pairs = (downs, quads, 2, rows, down_cols)
    mixed = pl.pallas_call(
        functools.partial(kernel, n),
        out_shape=landing,
        in_specs=[hbm] * 14,
        out_specs=(vmem, vmem),
        scratch_shapes=[pltpu.VMEM(a.shape, a.dtype) for a in landed]
        + [
            pltpu.VMEM((2, prefix_keys.shape[0], heads * DH), BF16),
            pltpu.VMEM((2, prefix_keys.shape[0], heads * DH), BF16),
            pltpu.VMEM((ups, width, up_cols), BF16),
            pltpu.VMEM((ups, width, up_cols), BF16),
            pltpu.VMEM((downs, hidden, down_cols), BF16),
            pltpu.VMEM((PREFIXES, 2, heads, slots, DH), BF16),
            pltpu.VMEM((n, heads, slots, DH), BF16),
            pltpu.VMEM((n, heads, slots, DH), BF16),
            pltpu.VMEM((n, heads, slots, DH), BF16),
            pltpu.VMEM((rows, width), F32),
            pltpu.VMEM((n, rows, width), BF16),
            pltpu.VMEM((ups, n * rows, up_cols), BF16),
            pltpu.VMEM(pairs, BF16),
            pltpu.VMEM(pairs, BF16),
            pltpu.VMEM(pairs, F32),
            pltpu.VMEM(pieces, BF16),
            pltpu.VMEM(pieces, BF16),
            pltpu.VMEM(pieces, F32),
            pltpu.VMEM(pieces, BF16),
            pltpu.VMEM(pieces, BF16),
            pltpu.SMEM(suffix_length.shape, jnp.int32),
            pltpu.SMEM((prefix_of.size,), jnp.int32),
            dma((9,)),
            dma((3,)),
            dma,
            dma,
            dma,
            dma,
            dma,
            dma,
            dma,
            dma,
            dma((n // 2,)),
            dma,
            dma,
            dma((downs,)),
            dma,
            dma((downs,)),
            dma,
            dma((downs,)),
        ],
        compiler_params=pltpu.CompilerParams(
            collective_id=0, has_side_effects=True, vmem_limit_bytes=52 * 2**20
        ),
    )(*placed)
    return tuple(
        pl.pallas_call(
            hand_over,
            out_shape=shapes,
            in_specs=[vmem] * 2,
            out_specs=(vmem, vmem),
            compiler_params=pltpu.CompilerParams(vmem_limit_bytes=2**20),
        )(*mixed)
    )


def solution(mesh):
    placed = (
        P(("groups", "wide"), None),
        P(("groups", "wide"), None),
        P(("groups", "wide"), None),
        P(("groups", "wide"), None),
        P(("groups", "wide"), None, None),
        P(("groups", "wide"), None, None),
        P(("groups", "wide")),
        P("groups", None),
        P("groups", None),
        P("groups", None),
        P(),
        P(None, "wide"),
        P(None, "wide"),
        P("wide", None),
    )
    return jax.shard_map(
        local,
        mesh=mesh,
        in_specs=placed,
        out_specs=(P(("groups", "wide"), None), P(("groups", "wide"), None)),
        check_vma=False,
    )
```
